128 devices in a mesh: gx: 8 (over x, core), gy: 16 (over z, y).
Axes of the slice: x: 4, y: 4, z: 4, core: 2. Of those that a mesh axis runs over, the one named last changes fastest.
Arguments:
- weights: float32 [2, 64, 16, 32, 512], P(None, None, 'gx', 'gy'), may hold values from -6 to 6
- interp: float32 [4, 4, 64, 64], replicated, may hold values from -0.375 to 0.375
- travel: float32 [64, 4096], replicated, may hold values from -3.140625 to 3.140625
- entry_rows: int32 [3, 8, 16, 2048], P(None, 'gx', 'gy'), may hold values from 0 to 4095
- exit_rows: int32 [3, 8, 16, 2048], P(None, 'gx', 'gy'), may hold values from 0 to 4095
Outputs:
- result: float32 [2, 64, 2, 4, 32768], P(None, None, None, None, ('gx', 'gy'))
The draws below stay inside these ranges and needn't reach their ends.
All inputs are finite; a program needn't handle non-finite values.
Results may differ from the reference program's by a relative error of at most 0.0001.
Values sent between devices are 32-bit elements; how exact they have to be, the bound alone decides.
No kernel may reach another device: no remote copies, remote signals or barrier semaphores. Data moves between devices by JAX's collectives and lax.ppermute only.
A program may use at most 128 MiB of HBM per device.

```python
import jax
import jax.numpy as jnp
import numpy as np
from jax import lax

Q = 64
TB0 = 512
NROW = 4096
PD = 2048
SX0 = 16
SY0 = 32
N_GX = 8
N_GY = 16


def place_ends(entries, key, low, largest):
    dims = entries.shape
    place = [jax.random.randint(jax.random.fold_in(key, axis), (), 0, dims[axis]) for axis in range(len(dims))]
    entries = entries.at[tuple(place)].set(low)
    longest = dims.index(max(dims))
    place[longest] = (place[longest] + 1) % dims[longest]
    return entries.at[tuple(place)].set(largest)


def shard_levels(rng, shape, shards, low, largest):
    factor_of, own = 1.0, jax.random.fold_in(rng, 6)
    for axis_at, shards_of in shards:
        draws = jnp.exp(jax.random.uniform(jax.random.fold_in(own, axis_at), (shards_of,), jnp.float32, low / len(shards), largest / len(shards)))
        factor_of = factor_of * jnp.repeat(draws, shape[axis_at] // shards_of).reshape([-1 if axis == axis_at else 1 for axis in range(len(shape))])
    return factor_of


def scatter_about(stream_key, shape, deviation, most, pieces=(), kind=jnp.bfloat16):
    factor_of = shard_levels(stream_key, shape, pieces, -0.22, 0.18) if pieces else 1.0
    drawn = jax.random.normal(stream_key, shape, jnp.float32) * deviation * factor_of
    return jnp.minimum(jnp.maximum(drawn, -most), most).astype(kind)


def setup_inputs(seed: int = 0) -> dict:
    keys = jax.random.split(jax.random.key(seed), 6)
    weights = scatter_about(keys[0], (2, Q, SX0, SY0, TB0), 1.0, 6.0, ((2, 8), (3, 16)), jnp.float32)
    interp = scatter_about(keys[1], (4, 4, Q, Q), (4 * Q) ** -0.5, 0.375, (), jnp.float32)
    travel = jnp.clip(jax.random.uniform(keys[2], (Q, NROW), jnp.float32, -3.140625, 3.140625), -3.140625, 3.140625)
    entry_rows = place_ends(jax.random.randint(keys[3], (3, N_GX, N_GY, PD), 0, NROW), jax.random.fold_in(keys[3], 1), 0, NROW - 1).astype(jnp.int32)
    exit_rows = place_ends(jax.random.randint(keys[4], (3, N_GX, N_GY, PD), 0, NROW), jax.random.fold_in(keys[4], 1), 0, NROW - 1).astype(jnp.int32)
    return dict(weights=weights, interp=interp, travel=travel, entry_rows=entry_rows, exit_rows=exit_rows)


highest = lax.Precision.HIGHEST


def rotate(fields, travel, row_index, sign):
    angles = jnp.take(travel, row_index, axis=1)
    cos_part = jnp.cos(angles)
    sin_part = jnp.sin(angles) * sign
    real_part = fields[0]
    imag_part = fields[1]
    return jnp.stack([cos_part * real_part - sin_part * imag_part, sin_part * real_part + cos_part * imag_part])


def combine(fields, interp, level_bit):
    x_bits = (np.arange(N_GX) >> level_bit) & 1
    y_bits = (np.arange(N_GY) >> level_bit) & 1
    target_child = 2 * x_bits[:, None] + y_bits[None, :]
    total = jnp.zeros(fields.shape, jnp.float32)
    for step_x in (0, 1):
        for step_y in (0, 1):
            x_peer = np.arange(N_GX) ^ (step_x << level_bit)
            y_peer = np.arange(N_GY) ^ (step_y << level_bit)
            moved = fields[:, :, x_peer][:, :, :, y_peer]
            source_child = 2 * x_bits[x_peer][:, None] + y_bits[y_peer][None, :]
            matrices = interp[target_child, source_child]
            total = total + jnp.einsum('ijts,rsijp->rtijp', matrices, moved, precision=highest)
    return total


def reference(weights, interp, travel, entry_rows, exit_rows):
    fields = weights.reshape(2, Q, N_GX, 2, N_GY, 2, TB0).transpose(0, 1, 2, 4, 3, 5, 6)
    fields = fields.reshape(2, Q, N_GX, N_GY, 4 * TB0)
    fields = rotate(fields, travel, entry_rows[0], -1.0)
    merged = jnp.einsum('kcts,rsijca->rtijka', interp, fields.reshape(2, Q, N_GX, N_GY, 4, TB0), precision=highest)
    fields = rotate(merged.reshape(2, Q, N_GX, N_GY, 4 * TB0), travel, exit_rows[0], 1.0)
    for section in (1, 2):
        fields = rotate(fields, travel, entry_rows[section], -1.0)
        fields = combine(fields, interp, section - 1)
        fields = rotate(fields, travel, exit_rows[section], 1.0)
    fields = fields.reshape(2, Q, N_GX // 4, 2, 2, N_GY // 4, 2, 2, 4, TB0)
    fields = fields.transpose(0, 1, 2, 5, 9, 8, 4, 7, 3, 6)
    return fields.reshape(2, Q, N_GX // 4, N_GY // 4, 64 * TB0)
```

```python
import jax
import jax.numpy as jnp
from jax import lax
from jax.sharding import PartitionSpec as P

high = lax.Precision.HIGH


def rotate(fields, angles):
    cos_part = jnp.cos(angles)
    sin_part = jnp.sin(angles)
    return jnp.stack(
        [
            cos_part * fields[0] - sin_part * fields[1],
            sin_part * fields[0] + cos_part * fields[1],
        ]
    )


def shards(weights, interp, travel, entry_rows, exit_rows):
    count = weights.shape[-1]
    points = interp.shape[-1]
    devices = lax.axis_size("gx") * lax.axis_size("gy")
    own = count // devices
    look = lambda rows: jnp.take(travel, rows, axis=1)
    matrix = interp.transpose(0, 2, 1, 3).reshape(4 * points, 4 * points)
    fields = weights.reshape(2, points, 4 * count)
    fields = rotate(fields, -look(entry_rows[0, 0, 0]))
    fields = jnp.einsum(
        "kcts,rsca->rtka", interp, fields.reshape(2, points, 4, count), precision=high
    ).reshape(2, points, 4 * count)
    fields = rotate(fields, look(exit_rows[0, 0, 0]) - look(entry_rows[1, 0, 0]))
    rows = jnp.stack([exit_rows[1, 0, 0], entry_rows[2, 0, 0], exit_rows[2, 0, 0]])
    payload = jnp.concatenate(
        [fields.reshape(2 * points, 4, devices, own), rows.astype(jnp.float32).reshape(3, 4, devices, own)]
    )
    payload = payload.transpose(2, 0, 1, 3).reshape(devices, 1, -1)
    moved = lax.all_to_all(payload, ("gx", "gy"), split_axis=0, concat_axis=0, tiled=True)
    moved = moved.reshape(devices, 2 * points + 3, 4 * own).transpose(1, 2, 0)
    angles = look(moved[2 * points :].astype(jnp.int32).reshape(3, -1))
    fields = moved[: 2 * points].reshape(2, points, 4 * own, 2, 2, 2, 4, 2, 2)
    blocks = interp.reshape(2, 2, 2, 2, points, points)
    fields = jnp.einsum("ijIJts,rsnXaIYbJ->rtnXaiYbj", blocks, fields, precision=high)
    fields = rotate(fields.reshape(2, points, -1), angles[:, 0] - angles[:, 1])
    fields = fields.reshape(2, points, 4 * own, 2, 2, 2, 4, 2, 2)
    fields = jnp.einsum("abABts,rsnXAiYBj->rtnXaiYbj", blocks, fields, precision=high)
    fields = rotate(fields.reshape(2, points, -1), angles[:, 2])
    fields = fields.reshape(2, points, 4, own, 2, 2, 2, 4, 2, 2)
    fields = fields.transpose(0, 1, 4, 7, 3, 2, 6, 9, 5, 8)
    return fields.reshape(2, points, 2, 4, -1)


def solution(mesh):
    return jax.shard_map(
        shards,
        mesh=mesh,
        in_specs=(
            P(None, None, "gx", "gy", None),
            P(),
            P(),
            P(None, "gx", "gy", None),
            P(None, "gx", "gy", None),
        ),
        out_specs=P(None, None, None, None, ("gx", "gy")),
        check_vma=False,
    )
```

```python
import jax
import jax.numpy as jnp
from jax import lax
from jax.experimental import pallas as pl
from jax.experimental.pallas import tpu as pltpu
from jax.sharding import PartitionSpec as P

LANES = 128
HALF = 64
CHUNK = 17
VMEM = pl.BlockSpec(memory_space=pltpu.VMEM)
SMEM = pl.BlockSpec(memory_space=pltpu.SMEM)


def cos_sin(x):
    turns = jnp.floor(x * 0.6366197723675814 + 0.5)
    r = x - turns * 1.5703125
    r = r - turns * 4.837512969970703e-4
    r = r - turns * 7.549789948768648e-8
    z = r * r
    s = r + r * z * ((-1.9515295891e-4 * z + 8.3321608736e-3) * z - 1.6666654611e-1)
    c = 1.0 - 0.5 * z + z * z * (
        (2.443315711809948e-5 * z - 1.388731625493765e-3) * z + 4.166664568298827e-2
    )
    q = turns.astype(jnp.int32)
    odd = (q & 1) == 1
    cos_part = jnp.where(odd, s, c)
    sin_part = jnp.where(odd, c, s)
    cos_part = jnp.where(((q + 1) & 2) == 2, -cos_part, cos_part)
    sin_part = jnp.where((q & 2) == 2, -sin_part, sin_part)
    return cos_part, sin_part


def swap(x):
    return pltpu.roll(x, HALF, 1)


def turn(state, wave, sign):
    low = lax.broadcasted_iota(jnp.int32, state.shape, 1) < HALF
    other = swap(wave)
    cos_part = jnp.where(low, wave, other)
    sin_part = jnp.where(low, other, wave)
    if sign > 0:
        sin_part = jnp.where(low, -sin_part, sin_part)
    else:
        sin_part = jnp.where(low, sin_part, -sin_part)
    return cos_part * state + sin_part * swap(state)


def split(x):
    high = x.astype(jnp.bfloat16)
    low = (x - high.astype(jnp.float32)).astype(jnp.bfloat16)
    return high, low


def product(x, high_ref, low_ref):
    dims = (((1,), (1,)), ((), ()))
    dot = lambda a, b: lax.dot_general(a, b, dims, preferred_element_type=jnp.float32)
    high, low = split(x)
    return dot(high, high_ref[...]) + (dot(high, low_ref[...]) + dot(low, high_ref[...]))


def gather(table, index, out, count, unroll):
    def body(step, carry):
        for n in range(unroll):
            at = step * unroll + n
            out[pl.ds(at, 1), :] = table[pl.ds(index(at), 1), :]
        return carry

    lax.fori_loop(0, count // unroll, body, 0)


def source_kernel(
    w_ref, interp_ref, travel_ref, entry_ref, exit_ref, rows_ref,
    out_ref, table_ref, high_ref, low_ref, wave0, wave1, wave2, rows_scratch,
):
    points = HALF
    zero = jnp.zeros((points, points), jnp.float32)
    for k in range(4):
        for c in range(4):
            block = interp_ref[k, c]
            full = jnp.concatenate(
                [jnp.concatenate([block, zero], 1), jnp.concatenate([zero, block], 1)], 0
            )
            high, low = split(full)
            high_ref[k * LANES : (k + 1) * LANES, c * LANES : (c + 1) * LANES] = high
            low_ref[k * LANES : (k + 1) * LANES, c * LANES : (c + 1) * LANES] = low

    def build(b, carry):
        at = pl.multiple_of(b * LANES, LANES)
        cos_part, sin_part = cos_sin(travel_ref[:, pl.ds(at, LANES)])
        table_ref[pl.ds(at, LANES), :] = jnp.concatenate([cos_part, sin_part], 0).T
        return carry

    lax.fori_loop(0, travel_ref.shape[1] // LANES, build, 0, unroll=2)
    slots = wave0.shape[0]
    gather(table_ref, lambda n: entry_ref[0, n], wave0, slots, 16)
    gather(table_ref, lambda n: exit_ref[0, n], wave1, slots, 16)
    gather(table_ref, lambda n: entry_ref[1, n], wave2, slots, 16)

    count = slots // 4
    lane = lax.broadcasted_iota(jnp.int32, (LANES, LANES), 1)
    rows_scratch[...] = rows_ref[...].astype(jnp.float32).T
    merged = rows_scratch[pl.ds(0, LANES, stride=4), :]
    for a in range(1, 4):
        part = pltpu.roll(rows_scratch[pl.ds(a, LANES, stride=4), :], 32 * a, 1)
        merged = jnp.where(lane >= 32 * a, part, merged)
    out_ref[pl.ds(16, LANES, stride=CHUNK), :] = merged

    for tile in range(count // LANES):
        parts = []
        for c in range(4):
            field = w_ref[pl.ds((c // 2) * 8 + tile * 2 + c % 2, LANES, stride=16), :].T
            wave = wave0[c * count + tile * LANES : c * count + (tile + 1) * LANES, :]
            parts.append(turn(field, wave, -1))
        merged = product(jnp.concatenate(parts, 1), high_ref, low_ref)
        for k in range(4):
            rows = slice(k * count + tile * LANES, k * count + (tile + 1) * LANES)
            field = merged[:, k * LANES : (k + 1) * LANES]
            field = turn(turn(field, wave1[rows, :], 1), wave2[rows, :], -1)
            for n in range(LANES // 4):
                at = (tile * (LANES // 4) + n) * CHUNK + k * 4
                out_ref[at : at + 4, :] = field[4 * n : 4 * n + 4, :]


def target_kernel(
    x_ref, table_ref, high_ref, low_ref,
    out_ref, rows_vmem, rows_smem, wave1, wave2, wave3, middle, last, sem,
):
    rows_vmem[...] = x_ref[pl.ds(16, LANES, stride=CHUNK), :].astype(jnp.int32)
    copy = pltpu.make_async_copy(rows_vmem, rows_smem, sem)
    copy.start()
    copy.wait()

    def body(source, carry):
        for e, wave in enumerate((wave1, wave2, wave3)):
            for k in range(4):
                for a in range(4):
                    row = rows_smem[source, a * 32 + e * 4 + k]
                    wave[pl.ds(source * 16 + k * 4 + a, 1), :] = table_ref[pl.ds(row, 1), :]
        return carry

    lax.fori_loop(0, LANES, body, 0)

    def place(sx, i1, i0, sy, j1, j0):
        return sx * 64 + i1 * 32 + i0 * 16 + sy * 4 + j1 * 2 + j0

    pairs = [(0, 0), (0, 1), (1, 0), (1, 1)]
    for sx in range(2):
        for i1 in range(2):
            outer = [(sy, j1) for sy in range(4) for j1 in range(2)]
            parts = [
                jnp.concatenate(
                    [
                        x_ref[place(sx, i1, i0, sy, j1, j0) * CHUNK : place(sx, i1, i0, sy, j1, j0) * CHUNK + 16, :]
                        for sy, j1 in outer
                    ],
                    0,
                )
                for i0, j0 in pairs
            ]
            merged = product(jnp.concatenate(parts, 1), high_ref, low_ref)
            for q, (i0, j0) in enumerate(pairs):
                for n, (sy, j1) in enumerate(outer):
                    at = place(sx, i1, i0, sy, j1, j0) * 16
                    field = merged[n * 16 : n * 16 + 16, q * LANES : (q + 1) * LANES]
                    field = turn(turn(field, wave1[at : at + 16, :], 1), wave2[at : at + 16, :], -1)
                    middle[at : at + 16, :] = field
    for sx in range(2):
        for i0 in range(2):
            outer = [(sy, j0) for sy in range(4) for j0 in range(2)]
            parts = [
                jnp.concatenate(
                    [
                        middle[place(sx, i1, i0, sy, j1, j0) * 16 : place(sx, i1, i0, sy, j1, j0) * 16 + 16, :]
                        for sy, j0 in outer
                    ],
                    0,
                )
                for i1, j1 in pairs
            ]
            merged = product(jnp.concatenate(parts, 1), high_ref, low_ref)
            for q, (i1, j1) in enumerate(pairs):
                for n, (sy, j0) in enumerate(outer):
                    at = place(sx, i1, i0, sy, j1, j0) * 16
                    field = merged[n * 16 : n * 16 + 16, q * LANES : (q + 1) * LANES]
                    field = turn(field, wave3[at : at + 16, :], 1)
                    group = (sx * 4 + sy) * 16 + i0 * 8 + j0 * 4 + i1 * 2 + j1
                    last[group * CHUNK : group * CHUNK + 16, :] = field
        for sy in range(4):
            base = (sx * 4 + sy) * 16 * CHUNK
            for half in range(2):
                pieces = [
                    last[pl.ds(base + k * 4 + a, 16, stride=CHUNK), :]
                    for a in (2 * half, 2 * half + 1)
                    for k in range(4)
                ]
                out_ref[pl.ds(sx * 8 + half * 4 + sy, LANES, stride=16), :] = jnp.concatenate(pieces, 0).T


def shards(weights, interp, travel, entry_rows, exit_rows):
    count = weights.shape[-1]
    points = interp.shape[-1]
    devices = lax.axis_size("gx") * lax.axis_size("gy")
    slots = 4 * count
    entry = entry_rows.reshape(3, slots)
    exits = exit_rows.reshape(3, slots)
    state = weights.reshape(2 * points, 2, 2, count // LANES, LANES)
    state = state.transpose(0, 1, 3, 2, 4).reshape(slots, LANES)
    rows = jnp.concatenate(
        [exits[1].reshape(4, count), entry[2].reshape(4, count), exits[2].reshape(4, count), jnp.zeros((LANES - 12, count), jnp.int32)]
    )
    f32 = lambda *shape: jax.ShapeDtypeStruct(shape, jnp.float32)
    wave = pltpu.VMEM((slots, LANES), jnp.float32)
    matrix = jax.ShapeDtypeStruct((4 * LANES, 4 * LANES), jnp.bfloat16)
    payload, table, high, low = pl.pallas_call(
        source_kernel,
        out_shape=[f32(devices * CHUNK, LANES), f32(travel.shape[1], LANES), matrix, matrix],
        in_specs=[VMEM, VMEM, VMEM, SMEM, SMEM, VMEM],
        out_specs=[VMEM] * 4,
        scratch_shapes=[wave, wave, wave, pltpu.VMEM((count, LANES), jnp.float32)],
        name="source",
    )(state, interp, travel, entry, exits, rows)
    moved = lax.all_to_all(
        payload.reshape(devices, 1, -1), ("gx", "gy"), split_axis=0, concat_axis=0, tiled=True
    )
    out = pl.pallas_call(
        target_kernel,
        out_shape=f32(slots, LANES),
        in_specs=[VMEM] * 4,
        out_specs=VMEM,
        scratch_shapes=[
            pltpu.VMEM((LANES, LANES), jnp.int32),
            pltpu.SMEM((LANES, LANES), jnp.int32),
            wave,
            wave,
            wave,
            wave,
            pltpu.VMEM((devices * CHUNK, LANES), jnp.float32),
            pltpu.SemaphoreType.DMA,
        ],
        name="target",
    )(moved.reshape(devices * CHUNK, LANES), table, high, low)
    out = out.reshape(2, points, 2, 2, 4, LANES).transpose(0, 1, 2, 4, 3, 5)
    return out.reshape(2, points, 2, 4, 2 * LANES)


def solution(mesh):
    return jax.shard_map(
        shards,
        mesh=mesh,
        in_specs=(
            P(None, None, "gx", "gy", None),
            P(),
            P(),
            P(None, "gx", "gy", None),
            P(None, "gx", "gy", None),
        ),
        out_specs=P(None, None, None, None, ("gx", "gy")),
        check_vma=False,
    )
```

```python
import jax
import jax.numpy as jnp
from jax import lax
from jax.experimental import pallas as pl
from jax.experimental.pallas import tpu as pltpu
from jax.sharding import PartitionSpec as P

LANES = 128
HALF = 64
CHUNK = 17
WIDE = 256
VMEM = pl.BlockSpec(memory_space=pltpu.VMEM)
HBM = pl.BlockSpec(memory_space=pltpu.HBM)
PIECES = 4


def cos_sin(x):
    z = x * x
    s = SIN[-1]
    for term in SIN[-2::-1]:
        s = s * z + term
    s = s * x
    c = COS[-1]
    for term in COS[-2::-1]:
        c = c * z + term
    return 1.0 - s * s, s * c


SIN = (0.70710677, -0.029462768, 3.682721e-4, -2.1885735e-6, 7.1936523e-9)
COS = (1.4142135, -0.17677669, 3.682845e-3, -3.0689214e-5, 1.3677929e-7, -3.5967443e-10)


def swap(x):
    return pltpu.roll(x, HALF, 1)


def low_half(x):
    return lax.broadcasted_iota(jnp.int32, x.shape, 1) < HALF


def interleave(first, second):
    low = low_half(first)
    return jnp.where(low, first, swap(second)), jnp.where(low, swap(first), second)


def modulate(wave, real, imag):
    cos_part, sin_part = wave
    return cos_part * real - sin_part * imag, sin_part * real + cos_part * imag


def demodulate(wave, real, imag):
    cos_part, sin_part = wave
    return cos_part * real + sin_part * imag, cos_part * imag - sin_part * real


def split(x):
    high = x.astype(jnp.bfloat16)
    low = (x - high.astype(jnp.float32)).astype(jnp.bfloat16)
    return high, low


def put(ref, row, block, x):
    high, low = split(x)
    for part, value in enumerate((high, low, high)):
        at = part * WIDE + block * LANES
        ref[pl.ds(row, x.shape[0]), at : at + LANES] = value


def dot(x_ref, matrix_ref, out_ref):
    out_ref[...] = jnp.dot(x_ref[...], matrix_ref[...], preferred_element_type=jnp.float32)


def source_kernel(
    w_hbm, interp_hbm, travel_hbm, entry_hbm, exit_hbm,
    out_ref, table_ref, matrix_ref,
    w_ref, interp_ref, travel_ref, entry_vmem, exit_vmem, entry_ref, exit_ref,
    wave0, wave1, wave2, rows_scratch, x_ref, merged, sems,
):
    width = travel_ref.shape[1] // PIECES
    piece = lambda p: (slice(None), slice(p * width, (p + 1) * width))
    copies = [
        pltpu.make_async_copy(travel_hbm.at[piece(p)], travel_ref.at[piece(p)], sems.at[p])
        for p in range(PIECES)
    ]
    operands = (
        (entry_hbm.at[:32], entry_ref),
        (exit_hbm.at[:16], exit_ref),
        (w_hbm, w_ref),
        (interp_hbm, interp_ref),
        (entry_hbm, entry_vmem),
        (exit_hbm, exit_vmem),
    )
    copies += [
        pltpu.make_async_copy(*pair, sems.at[PIECES + n]) for n, pair in enumerate(operands)
    ]
    for copy in copies:
        copy.start()

    def build(b, carry):
        at = pl.multiple_of(b * LANES, LANES)
        cos_part, sin_part = cos_sin(travel_ref[:, pl.ds(at, LANES)])
        table_ref[pl.ds(at, LANES), :] = jnp.concatenate([cos_part, sin_part], 0).T
        return carry

    blocks = width // LANES
    for p in range(PIECES):
        copies[p].wait()
        lax.fori_loop(p * blocks, (p + 1) * blocks, build, 0, unroll=4)
    for copy in copies[PIECES : PIECES + 2]:
        copy.wait()

    def gather(step, carry):
        at = step * LANES
        for n in range(LANES):
            wave0[pl.ds(at + n, 1), :] = table_ref[pl.ds(entry_ref[step, n], 1), :]
            wave1[pl.ds(at + n, 1), :] = table_ref[pl.ds(exit_ref[step, n], 1), :]
            wave2[pl.ds(at + n, 1), :] = table_ref[pl.ds(entry_ref[step + 16, n], 1), :]
        return carry

    lax.fori_loop(0, wave0.shape[0] // LANES, gather, 0)
    for copy in copies[PIECES + 2 :]:
        copy.wait()

    for kp in range(2):
        for cp in range(2):
            rows = [
                jnp.concatenate([interp_ref[2 * kp + kk, 2 * cp], interp_ref[2 * kp + kk, 2 * cp + 1]], 1)
                for kk in range(2)
            ]
            high, low = split(jnp.concatenate(rows, 0).T)
            for part, value in enumerate((high, high, low)):
                at = part * WIDE + cp * LANES
                matrix_ref[at : at + LANES, kp * LANES : (kp + 1) * LANES] = value

    tiles = rows_scratch.shape[0] // LANES
    zero = jnp.zeros((LANES - 12, LANES), jnp.float32)
    for tile in range(tiles):
        rows = [
            exit_vmem[pl.ds(16 + tile, 8, stride=tiles), :].astype(jnp.float32),
            entry_vmem[pl.ds(32 + tile, 4, stride=tiles), :].astype(jnp.float32),
            zero,
        ]
        rows_scratch[tile * LANES : (tile + 1) * LANES, :] = jnp.concatenate(rows, 0).T
    lane = lax.broadcasted_iota(jnp.int32, (LANES, LANES), 1)
    indices = rows_scratch[pl.ds(0, LANES, stride=4), :]
    for a in range(1, 4):
        part = pltpu.roll(rows_scratch[pl.ds(a, LANES, stride=4), :], 16 * a, 1)
        indices = jnp.where(lane >= 16 * a, part, indices)
    out_ref[pl.ds(16, LANES, stride=CHUNK), :] = indices

    count = tiles * LANES

    def pair(wave, p, at):
        return interleave(
            *[wave[pl.ds(pl.multiple_of(n * count + at, LANES), LANES), :] for n in (2 * p, 2 * p + 1)]
        )

    def enter(tile, carry):
        at = pl.multiple_of(tile * LANES, LANES)
        for cx in range(2):
            parts = []
            for r in range(2):
                start = r * HALF * 16 + cx * 8 + tile * 2
                block = [w_ref[pl.ds(start + cy, HALF, stride=16), :] for cy in range(2)]
                parts.append(jnp.concatenate(block, 0).T)
            real, imag = demodulate(pair(wave0, cx, at), *parts)
            put(x_ref, at, cx, real)
            put(x_ref, pl.multiple_of(count + at, LANES), cx, imag)
        return carry

    lax.fori_loop(0, tiles, enter, 0)
    dot(x_ref, matrix_ref, merged)

    def leave(tile, carry):
        at = pl.multiple_of(tile * LANES, LANES)
        sent = out_ref.at[pl.ds(pl.multiple_of(tile * (LANES // 4) * CHUNK, 8), (LANES // 4) * CHUNK), :]
        for kp in range(2):
            block = slice(kp * LANES, (kp + 1) * LANES)
            real = merged[pl.ds(at, LANES), block]
            imag = merged[pl.ds(pl.multiple_of(count + at, LANES), LANES), block]
            fields = modulate(pair(wave1, kp, at), real, imag)
            fields = demodulate(pair(wave2, kp, at), *fields)
            for r in range(2):
                for n in range(LANES // 4):
                    to = n * CHUNK + r * 8 + kp * 4
                    sent[to : to + 4, :] = fields[r][4 * n : 4 * n + 4, :]
        return carry

    lax.fori_loop(0, tiles, leave, 0)


def target_kernel(
    x_ref, table_ref, matrix_ref,
    out_ref, rows_vmem, rows_smem, wave1, wave2, wave3, x1_ref, x2_ref, merged, last, sems,
):
    count = rows_vmem.shape[0]
    indices = [x_ref[pl.ds(16 + n * CHUNK, count, stride=2 * CHUNK), :] for n in range(2)]
    rows_vmem[...] = jnp.where(low_half(indices[0]), indices[0], swap(indices[1])).astype(jnp.int32)
    size = count // PIECES
    copies = []
    for p in range(PIECES):
        part = slice(p * size, (p + 1) * size)
        copies.append(pltpu.make_async_copy(rows_vmem.at[part], rows_smem.at[part], sems.at[p]))
        copies[-1].start()

    bits = range(2)

    def first(step, carry):
        base = 32 * CHUNK
        part = x_ref.at[pl.ds(pl.multiple_of(step * base, 8), base), :]
        for sy in range(4):
            for j1 in bits:
                group = pl.multiple_of(step * 256 + (sy * 2 + j1) * 32, 32)
                for i0 in bits:
                    at = [(i0 * 16 + sy * 4 + j1 * 2 + j0) * CHUNK for j0 in bits]
                    parts = interleave(*[part[a : a + 16, :] for a in at])
                    rows = [parts[kk][8 * r : 8 * r + 8] for r in bits for kk in bits]
                    put(x1_ref, group, i0, jnp.concatenate(rows, 0))
        return carry

    lax.fori_loop(0, 4, first, 0)
    dot(x1_ref, matrix_ref, merged)

    def gather(row, carry):
        for n in range(2):
            for e, wave in enumerate((wave1, wave3, wave2)):
                for k in range(4):
                    for a in range(4):
                        index = rows_smem[row, n * HALF + a * 16 + e * 4 + k]
                        at = row * 32 + n * 16 + (k % 2) * 8 + (k // 2) * 4 + a
                        wave[pl.ds(at, 1), :] = table_ref[pl.ds(index, 1), :]
        return carry

    for p in range(PIECES):
        copies[p].wait()
        lax.fori_loop(p * size, (p + 1) * size, gather, 0)

    def rows_of(ref, base, offset, block=slice(None), size=16):
        return ref[pl.ds(pl.multiple_of(base + offset, 16), size), block]

    def second(n, carry):
        sx, sy = n // 4, n % 4
        ends = (sx * 64 + sy * 4) * 16
        for i1 in bits:
            for i0 in bits:
                fields = []
                for j1 in bits:
                    group = sx * 512 + sy * 64
                    offset = i1 * 256 + j1 * 32
                    block = slice(i0 * LANES, (i0 + 1) * LANES)
                    field = [rows_of(merged, group, offset + r * 16, block) for r in bits]
                    pair = [
                        interleave(
                            *[rows_of(wave, ends, (i1 * 32 + i0 * 16 + j1 * 2 + j0) * 16) for j0 in bits]
                        )
                        for wave in (wave1, wave2)
                    ]
                    field = modulate(pair[0], *field)
                    fields.append(demodulate(pair[1], *field))
                for r in bits:
                    parts = interleave(fields[0][r], fields[1][r])
                    for j0 in bits:
                        put(x2_ref, pl.multiple_of(n * 128 + (i0 * 2 + j0) * 32 + r * 16, 16), i1, parts[j0])
        return carry

    lax.fori_loop(0, 8, second, 0)
    dot(x2_ref, matrix_ref, merged)

    def third(n, carry):
        sx, sy = n // 4, n % 4
        ends = (sx * 64 + sy * 4) * 16
        for i0 in bits:
            for j0 in bits:
                for i1 in bits:
                    block = slice(i1 * LANES, (i1 + 1) * LANES)
                    field = [
                        rows_of(merged, n * 128, (i0 * 2 + j0) * 32 + r * 16, block) for r in bits
                    ]
                    pair = interleave(
                        *[rows_of(wave3, ends, (i1 * 32 + i0 * 16 + j1 * 2 + j0) * 16) for j1 in bits]
                    )
                    field = interleave(*modulate(pair, *field))
                    for j1 in bits:
                        at = (i0 * 8 + j0 * 4 + i1 * 2 + j1) * CHUNK
                        last[at : at + 16, :] = field[j1]
        for half in bits:
            pieces = [
                last[pl.ds((k % 2) * 8 + (k // 2) * 4 + a, 16, stride=CHUNK), :]
                for a in (2 * half, 2 * half + 1)
                for k in range(4)
            ]
            out_ref[pl.ds(sx * 8 + half * 4 + sy, LANES, stride=16), :] = jnp.concatenate(pieces, 0).T
        return carry

    lax.fori_loop(0, 8, third, 0)


def shards(weights, interp, travel, entry_rows, exit_rows):
    count = weights.shape[-1]
    points = interp.shape[-1]
    devices = lax.axis_size("gx") * lax.axis_size("gy")
    slots = 4 * count
    entry = entry_rows.reshape(3 * slots // LANES, LANES)
    exits = exit_rows.reshape(3 * slots // LANES, LANES)
    state = weights.reshape(2 * points, 2, 2, count // LANES, LANES)
    state = state.transpose(0, 1, 3, 2, 4).reshape(slots, LANES)
    f32 = lambda *shape: jax.ShapeDtypeStruct(shape, jnp.float32)
    vmem = lambda *shape: pltpu.VMEM(shape, jnp.float32)
    left = pltpu.VMEM((slots // 2, 3 * WIDE), jnp.bfloat16)
    params = pltpu.CompilerParams(vmem_limit_bytes=28 << 20)
    payload, table, matrix = pl.pallas_call(
        source_kernel,
        out_shape=[
            f32(devices * CHUNK, LANES),
            f32(travel.shape[1], LANES),
            jax.ShapeDtypeStruct((3 * WIDE, WIDE), jnp.bfloat16),
        ],
        in_specs=[HBM] * 5,
        out_specs=[VMEM] * 3,
        scratch_shapes=[
            vmem(slots, LANES),
            vmem(*interp.shape),
            vmem(*travel.shape),
            pltpu.VMEM(entry.shape, jnp.int32),
            pltpu.VMEM(exits.shape, jnp.int32),
            pltpu.SMEM((32, LANES), jnp.int32),
            pltpu.SMEM((16, LANES), jnp.int32),
            vmem(slots, LANES),
            vmem(slots, LANES),
            vmem(slots, LANES),
            vmem(count, LANES),
            left,
            vmem(slots // 2, WIDE),
            pltpu.SemaphoreType.DMA((PIECES + 6,)),
        ],
        compiler_params=params,
        name="source",
    )(*[pltpu.with_memory_space_constraint(x, pltpu.HBM) for x in (state, interp, travel, entry, exits)])
    moved = lax.all_to_all(
        payload.reshape(devices, 1, -1), ("gx", "gy"), split_axis=0, concat_axis=0, tiled=True
    )
    out = pl.pallas_call(
        target_kernel,
        out_shape=f32(slots, LANES),
        in_specs=[VMEM] * 3,
        out_specs=VMEM,
        scratch_shapes=[
            pltpu.VMEM((HALF, LANES), jnp.int32),
            pltpu.SMEM((HALF, LANES), jnp.int32),
            vmem(slots, LANES),
            vmem(slots, LANES),
            vmem(slots, LANES),
            left,
            left,
            vmem(slots // 2, WIDE),
            vmem(16 * CHUNK, LANES),
            pltpu.SemaphoreType.DMA((PIECES,)),
        ],
        compiler_params=params,
        name="target",
    )(moved.reshape(devices * CHUNK, LANES), table, matrix)
    out = out.reshape(2, points, 2, 2, 4, LANES).transpose(0, 1, 2, 4, 3, 5)
    return out.reshape(2, points, 2, 4, 2 * LANES)


def solution(mesh):
    return jax.shard_map(
        shards,
        mesh=mesh,
        in_specs=(
            P(None, None, "gx", "gy", None),
            P(),
            P(),
            P(None, "gx", "gy", None),
            P(None, "gx", "gy", None),
        ),
        out_specs=P(None, None, None, None, ("gx", "gy")),
        check_vma=False,
    )
```

```python
import jax
import jax.numpy as jnp
from jax import lax
from jax.experimental import pallas as pl
from jax.experimental.pallas import tpu as pltpu
from jax.sharding import PartitionSpec as P

LANES = 128
HALF = 64
CHUNK = 17
WIDE = 256
VMEM = pl.BlockSpec(memory_space=pltpu.VMEM)
HBM = pl.BlockSpec(memory_space=pltpu.HBM)
PIECES = 4


def cos_sin(x):
    z = x * x
    s = SIN[-1]
    for term in SIN[-2::-1]:
        s = s * z + term
    s = s * x
    c = COS[-1]
    for term in COS[-2::-1]:
        c = c * z + term
    return 1.0 - s * s, s * c


SIN = (0.70710677, -0.029462768, 3.682721e-4, -2.1885735e-6, 7.1936523e-9)
COS = (1.4142135, -0.17677669, 3.682845e-3, -3.0689214e-5, 1.3677929e-7, -3.5967443e-10)


def swap(x):
    return pltpu.roll(x, HALF, 1)


def low_half(x):
    return lax.broadcasted_iota(jnp.int32, x.shape, 1) < HALF


def interleave(first, second):
    low = low_half(first)
    moved = swap(jnp.where(low, second, first))
    return jnp.where(low, first, moved), jnp.where(low, moved, second)


def modulate(wave, real, imag):
    cos_part, sin_part = wave
    return cos_part * real - sin_part * imag, sin_part * real + cos_part * imag


def demodulate(wave, real, imag):
    cos_part, sin_part = wave
    return cos_part * real + sin_part * imag, cos_part * imag - sin_part * real


def split(x):
    high = x.astype(jnp.bfloat16)
    low = (x - high.astype(jnp.float32)).astype(jnp.bfloat16)
    return high, low


def put(ref, row, block, x):
    high, low = split(x)
    for part, value in enumerate((high, low, high)):
        at = part * WIDE + block * LANES
        ref[pl.ds(row, x.shape[0]), at : at + LANES] = value


def dot(x_ref, matrix_ref, between=lambda: None):
    total = None
    for part in range(3):
        at = slice(part * WIDE, (part + 1) * WIDE)
        term = jnp.dot(x_ref[:, at], matrix_ref[at, :], preferred_element_type=jnp.float32)
        total = term if total is None else total + term
        between()
    return total


def source_kernel(
    w_hbm, interp_hbm, travel_hbm, entry_hbm, exit_hbm, entry_rows_hbm, exit_rows_hbm,
    out_ref, table_ref, matrix_ref,
    w_ref, interp_ref, travel_ref, entry_vmem, exit_vmem, entry_ref, exit_ref, next_ref,
    wave0, wave1, wave2, rows_scratch, x_ref, merged, sems,
):
    slots = wave0.shape[0]
    width = travel_ref.shape[1] // PIECES

    def piece(p):
        at = (slice(None), pl.ds(pl.multiple_of(p * width, width), width))
        return pltpu.make_async_copy(travel_hbm.at[at], travel_ref.at[at], sems.at[p])

    operands = (
        (interp_hbm, interp_ref),
        (entry_rows_hbm, entry_vmem),
        (exit_rows_hbm, exit_vmem),
        (entry_hbm.at[:slots], entry_ref),
        (exit_hbm.at[:slots], exit_ref),
        (entry_hbm.at[slots : 2 * slots], next_ref),
        (w_hbm, w_ref),
    )
    copies = [
        pltpu.make_async_copy(*pair, sems.at[PIECES + n]) for n, pair in enumerate(operands)
    ]
    for copy in copies[:3]:
        copy.start()
    for p in range(PIECES):
        piece(p).start()
    for copy in copies[3:]:
        copy.start()

    for copy in copies[:3]:
        copy.wait()
    for kp in range(2):
        for cp in range(2):
            rows = [
                jnp.concatenate([interp_ref[2 * kp + kk, 2 * cp], interp_ref[2 * kp + kk, 2 * cp + 1]], 1)
                for kk in range(2)
            ]
            high, low = split(jnp.concatenate(rows, 0).T)
            for part, value in enumerate((high, high, low)):
                at = part * WIDE + cp * LANES
                matrix_ref[at : at + LANES, kp * LANES : (kp + 1) * LANES] = value

    tiles = rows_scratch.shape[0] // LANES
    for tile in range(tiles):
        rows = []
        for ref, e in ((exit_vmem, 1), (entry_vmem, 2), (exit_vmem, 2)):
            rows.append(ref[pl.ds(16 * e + tile, 4, stride=tiles), :].astype(jnp.float32))
            rows.append(jnp.zeros((12, LANES), jnp.float32))
        rows.append(jnp.zeros((LANES - 48, LANES), jnp.float32))
        rows_scratch[tile * LANES : (tile + 1) * LANES, :] = jnp.concatenate(rows, 0).T
    lane = lax.broadcasted_iota(jnp.int32, (LANES, LANES), 1)
    indices = rows_scratch[pl.ds(0, LANES, stride=4), :]
    for a in range(1, 4):
        part = pltpu.roll(rows_scratch[pl.ds(a, LANES, stride=4), :], 4 * a, 1)
        indices = jnp.where((lane & 15) >= 4 * a, part, indices)
    out_ref[pl.ds(16, LANES, stride=CHUNK), :] = indices

    def build(p, carry):
        piece(p).wait()

        def block(b, carry):
            at = pl.multiple_of(p * width + b * 2 * LANES, 2 * LANES)
            cos_part, sin_part = cos_sin(travel_ref[:, pl.ds(at, 2 * LANES)])
            table_ref[pl.ds(at, 2 * LANES), :] = jnp.concatenate([cos_part, sin_part], 0).T
            return carry

        return lax.fori_loop(0, width // (2 * LANES), block, carry)

    lax.fori_loop(0, PIECES, build, 0)
    for copy in copies[3:]:
        copy.wait()

    size = 64

    def gather(step, carry):
        at = step * size
        for n in range(size):
            wave0[pl.ds(at + n, 1), :] = table_ref[pl.ds(entry_ref[at + n], 1), :]
        return carry

    lax.fori_loop(0, slots // size, gather, 0)

    count = tiles * LANES

    def pair(wave, p, at):
        return interleave(
            *[wave[pl.ds(pl.multiple_of(n * count + at, LANES), LANES), :] for n in (2 * p, 2 * p + 1)]
        )

    def enter(tile, carry):
        at = pl.multiple_of(tile * LANES, LANES)
        chunks = iter(range(8))

        def between():
            base = tile * 4 * LANES + next(chunks) * HALF
            for n in range(HALF):
                wave1[pl.ds(base + n, 1), :] = table_ref[pl.ds(exit_ref[base + n], 1), :]
                wave2[pl.ds(base + n, 1), :] = table_ref[pl.ds(next_ref[base + n], 1), :]

        for cx in range(2):
            parts = []
            for r in range(2):
                start = r * HALF * 16 + cx * 8 + tile * 2
                block = [w_ref[pl.ds(start + cy, HALF, stride=16), :] for cy in range(2)]
                parts.append(jnp.concatenate(block, 0).T)
            between()
            real, imag = demodulate(pair(wave0, cx, at), *parts)
            put(x_ref, 0, cx, real)
            put(x_ref, LANES, cx, imag)
            between()
        between()
        merged[pl.ds(pl.multiple_of(tile * WIDE, WIDE), WIDE), :] = dot(x_ref, matrix_ref, between)
        return carry

    lax.fori_loop(0, tiles, enter, 0)

    def leave(tile, carry):
        at = pl.multiple_of(tile * LANES, LANES)
        sent = out_ref.at[pl.ds(pl.multiple_of(tile * (LANES // 4) * CHUNK, 8), (LANES // 4) * CHUNK), :]
        for kp in range(2):
            block = slice(kp * LANES, (kp + 1) * LANES)
            real, imag = [
                merged[pl.ds(pl.multiple_of(tile * WIDE + r * LANES, LANES), LANES), block] for r in range(2)
            ]
            fields = modulate(pair(wave1, kp, at), real, imag)
            fields = demodulate(pair(wave2, kp, at), *fields)
            for r in range(2):
                for n in range(LANES // 4):
                    to = n * CHUNK + r * 8 + kp * 4
                    sent[to : to + 4, :] = fields[r][4 * n : 4 * n + 4, :]
        return carry

    lax.fori_loop(0, tiles, leave, 0)


def target_kernel(
    x_ref, table_ref, matrix_ref,
    out_ref, rows_vmem, waves, more_waves, x1_ref, x2_ref, merged, result, last, sems, *rows_smem,
):
    rows_vmem[...] = x_ref[pl.ds(16, LANES, stride=CHUNK), :].astype(jnp.int32).T
    copies = [
        pltpu.make_async_copy(rows_vmem.at[pl.ds(n, 1), :], to, sems.at[n]) for n, to in enumerate(rows_smem)
    ]
    for copy in copies:
        copy.start()

    bits = range(2)

    def first(step, carry):
        base = 32 * CHUNK
        part = x_ref.at[pl.ds(pl.multiple_of(step * base, 8), base), :]
        for sy in range(4):
            for j1 in bits:
                group = pl.multiple_of(step * 256 + (sy * 2 + j1) * 32, 32)
                for i0 in bits:
                    at = [(i0 * 16 + sy * 4 + j1 * 2 + j0) * CHUNK for j0 in bits]
                    parts = interleave(*[part[a : a + 16, :] for a in at])
                    rows = [parts[kk][8 * r : 8 * r + 8] for r in bits for kk in bits]
                    put(x1_ref, group, i0, jnp.concatenate(rows, 0))
        return carry

    lax.fori_loop(0, 4, first, 0)

    merged[:512, :] = dot(x1_ref.at[:512, :], matrix_ref)
    for copy in copies:
        copy.wait()

    def gather(n, wave):
        base = n // 4 * 64 + n % 4 * 4
        chunks = iter(range(16))

        def chunk():
            b = next(chunks)
            source = base + (b >> 2) * 16 + b % 4
            for e in range(3):
                for k in range(4):
                    for a in range(4):
                        index = rows_smem[e * 16 + a * 4 + k][0, source]
                        at = e * 256 + b * 16 + k % 2 * 8 + k // 2 * 4 + a
                        wave[at : at + 1, :] = table_ref[pl.ds(index, 1), :]

        return chunk

    def levels(n, wave, between):
        sx, sy = n // 4, n % 4

        def pair(to, ends):
            at = [to * 256 + ((i1 * 2 + i0) * 4 + j1 * 2 + j0) * 16 for i1, i0, j1, j0 in ends]
            return interleave(*[wave[a : a + 16, :] for a in at])

        for i1 in bits:
            for i0 in bits:
                fields = []
                block = slice(i0 * LANES, (i0 + 1) * LANES)
                for j1 in bits:
                    group = sx * 512 + sy * 64 + i1 * 256 + j1 * 32
                    field = [
                        merged[pl.ds(pl.multiple_of(group + r * 16, 16), 16), block] for r in bits
                    ]
                    ends = [(i1, i0, j1, j0) for j0 in bits]
                    field = modulate(pair(0, ends), *field)
                    fields.append(demodulate(pair(1, ends), *field))
                for r in bits:
                    parts = interleave(fields[0][r], fields[1][r])
                    for j0 in bits:
                        put(x2_ref, (i0 * 2 + j0) * 32 + r * 16, i1, parts[j0])
                    between()
        result[...] = dot(x2_ref, matrix_ref, between)
        for i0 in bits:
            for j0 in bits:
                for i1 in bits:
                    block = slice(i1 * LANES, (i1 + 1) * LANES)
                    group = (i0 * 2 + j0) * 32
                    field = [result[group + r * 16 : group + r * 16 + 16, block] for r in bits]
                    field = interleave(*modulate(pair(2, [(i1, i0, j1, j0) for j1 in bits]), *field))
                    for j1 in bits:
                        at = (i0 * 8 + j0 * 4 + i1 * 2 + j1) * CHUNK
                        last[at : at + 16, :] = field[j1]
                between()
        for half in bits:
            pieces = [
                last[pl.ds((k % 2) * 8 + (k // 2) * 4 + a, 16, stride=CHUNK), :]
                for a in (2 * half, 2 * half + 1)
                for k in range(4)
            ]
            out_ref[pl.ds(sx * 8 + half * 4 + sy, LANES, stride=16), :] = jnp.concatenate(pieces, 0).T
            if half == 0:
                between()

    chunk = gather(0, waves)

    def some():
        for _ in range(5):
            chunk()

    merged[512:, :] = dot(x1_ref.at[512:, :], matrix_ref, some)
    chunk()

    def two(m, carry):
        levels(2 * m, waves, gather(2 * m + 1, more_waves))
        levels(2 * m + 1, more_waves, gather((2 * m + 2) % 8, waves))
        return carry

    lax.fori_loop(0, 4, two, 0)


def shards(weights, interp, travel, entry_rows, exit_rows):
    count = weights.shape[-1]
    points = interp.shape[-1]
    devices = lax.axis_size("gx") * lax.axis_size("gy")
    slots = 4 * count
    entry = entry_rows.reshape(3 * slots // LANES, LANES)
    exits = exit_rows.reshape(3 * slots // LANES, LANES)
    state = weights.reshape(2 * points, 2, 2, count // LANES, LANES)
    state = state.transpose(0, 1, 3, 2, 4).reshape(slots, LANES)
    f32 = lambda *shape: jax.ShapeDtypeStruct(shape, jnp.float32)
    vmem = lambda *shape: pltpu.VMEM(shape, jnp.float32)
    params = pltpu.CompilerParams(vmem_limit_bytes=28 << 20)
    operands = state, interp, travel, entry_rows.reshape(-1), exit_rows.reshape(-1), entry, exits
    payload, table, matrix = pl.pallas_call(
        source_kernel,
        out_shape=[
            f32(devices * CHUNK, LANES),
            f32(travel.shape[1], LANES),
            jax.ShapeDtypeStruct((3 * WIDE, WIDE), jnp.bfloat16),
        ],
        in_specs=[HBM] * 7,
        out_specs=[VMEM] * 3,
        scratch_shapes=[
            vmem(slots, LANES),
            vmem(*interp.shape),
            vmem(*travel.shape),
            pltpu.VMEM(entry.shape, jnp.int32),
            pltpu.VMEM(exits.shape, jnp.int32),
            pltpu.SMEM((slots,), jnp.int32),
            pltpu.SMEM((slots,), jnp.int32),
            pltpu.SMEM((slots,), jnp.int32),
            vmem(slots, LANES),
            vmem(slots, LANES),
            vmem(slots, LANES),
            vmem(count, LANES),
            pltpu.VMEM((WIDE, 3 * WIDE), jnp.bfloat16),
            vmem(slots // 2, WIDE),
            pltpu.SemaphoreType.DMA((PIECES + 7,)),
        ],
        compiler_params=params,
        name="source",
    )(*[pltpu.with_memory_space_constraint(x, pltpu.HBM) for x in operands])
    moved = lax.all_to_all(
        payload.reshape(devices, 1, -1), ("gx", "gy"), split_axis=0, concat_axis=0, tiled=True
    )
    out = pl.pallas_call(
        target_kernel,
        out_shape=f32(slots, LANES),
        in_specs=[VMEM] * 3,
        out_specs=VMEM,
        scratch_shapes=[
            pltpu.VMEM((LANES, LANES), jnp.int32),
            vmem(3 * 256, LANES),
            vmem(3 * 256, LANES),
            pltpu.VMEM((slots // 2, 3 * WIDE), jnp.bfloat16),
            pltpu.VMEM((LANES, 3 * WIDE), jnp.bfloat16),
            vmem(slots // 2, WIDE),
            vmem(LANES, WIDE),
            vmem(16 * CHUNK, LANES),
            pltpu.SemaphoreType.DMA((48,)),
        ]
        + [pltpu.SMEM((1, LANES), jnp.int32)] * 48,
        compiler_params=params,
        name="target",
    )(moved.reshape(devices * CHUNK, LANES), table, matrix)
    out = out.reshape(2, points, 2, 2, 4, LANES).transpose(0, 1, 2, 4, 3, 5)
    return out.reshape(2, points, 2, 4, 2 * LANES)


def solution(mesh):
    return jax.shard_map(
        shards,
        mesh=mesh,
        in_specs=(
            P(None, None, "gx", "gy", None),
            P(),
            P(),
            P(None, "gx", "gy", None),
            P(None, "gx", "gy", None),
        ),
        out_specs=P(None, None, None, None, ("gx", "gy")),
        check_vma=False,
    )
```

```python
import jax
import jax.numpy as jnp
from jax import lax
from jax.experimental import pallas as pl
from jax.experimental.pallas import tpu as pltpu
from jax.sharding import PartitionSpec as P

LANES = 128
HALF = 64
CHUNK = 17
WIDE = 256
VMEM = pl.BlockSpec(memory_space=pltpu.VMEM)
HBM = pl.BlockSpec(memory_space=pltpu.HBM)
PIECES = 4


def cos_sin(x):
    z = x * x
    s = SIN[-1]
    for term in SIN[-2::-1]:
        s = s * z + term
    s = s * x
    c = COS[-1]
    for term in COS[-2::-1]:
        c = c * z + term
    return 1.0 - s * s, s * c


SIN = (0.70710677, -0.029462768, 3.682721e-4, -2.1885735e-6, 7.1936523e-9)
COS = (1.4142135, -0.17677669, 3.682845e-3, -3.0689214e-5, 1.3677929e-7, -3.5967443e-10)


def swap(x):
    return pltpu.roll(x, HALF, 1)


def low_half(x):
    return lax.broadcasted_iota(jnp.int32, x.shape, 1) < HALF


def interleave(first, second):
    low = low_half(first)
    moved = swap(jnp.where(low, second, first))
    return jnp.where(low, first, moved), jnp.where(low, moved, second)


def modulate(wave, real, imag):
    cos_part, sin_part = wave
    return cos_part * real - sin_part * imag, sin_part * real + cos_part * imag


def demodulate(wave, real, imag):
    cos_part, sin_part = wave
    return cos_part * real + sin_part * imag, cos_part * imag - sin_part * real


def split(x):
    high = x.astype(jnp.bfloat16)
    low = (x - high.astype(jnp.float32)).astype(jnp.bfloat16)
    return high, low


def put(ref, row, block, x):
    high, low = split(x)
    for part, value in enumerate((high, low, high)):
        at = part * WIDE + block * LANES
        ref[pl.ds(row, x.shape[0]), at : at + LANES] = value


def dot(x_ref, matrix_ref, between=lambda: None):
    total = None
    for part in range(3):
        at = slice(part * WIDE, (part + 1) * WIDE)
        term = jnp.dot(x_ref[:, at], matrix_ref[at, :], preferred_element_type=jnp.float32)
        total = term if total is None else total + term
        between()
    return total


def source_kernel(
    w_hbm, interp_hbm, travel_hbm, entry_hbm, exit_hbm,
    out_ref, table_ref, matrix_ref,
    w_ref, interp_ref, travel_ref, entry_vmem, exit_vmem,
    wave0, wave1, wave2, rows_scratch, x_ref, merged, sems, *index_refs,
):
    groups = wave0.shape[0] // LANES
    width = travel_ref.shape[1] // PIECES

    def piece(p):
        at = (slice(None), pl.ds(pl.multiple_of(p * width, width), width))
        return pltpu.make_async_copy(travel_hbm.at[at], travel_ref.at[at], sems.at[p])

    operands = (
        (interp_hbm, interp_ref),
        (entry_hbm, entry_vmem),
        (exit_hbm, exit_vmem),
        (w_hbm, w_ref),
    )
    rows = [(entry_hbm, n) for n in range(groups)] + [(exit_hbm, n) for n in range(groups)]
    rows += [(entry_hbm, groups + n) for n in range(groups)]
    operands += tuple((ref.at[pl.ds(n, 1), :], to) for (ref, n), to in zip(rows, index_refs))
    entry_refs, exit_refs, next_refs = [index_refs[n * groups : (n + 1) * groups] for n in range(3)]
    copies = [
        pltpu.make_async_copy(*pair, sems.at[PIECES + n]) for n, pair in enumerate(operands)
    ]
    for copy in copies[:3]:
        copy.start()
    for p in range(PIECES):
        piece(p).start()
    for copy in copies[3:]:
        copy.start()

    for copy in copies[:3]:
        copy.wait()
    for kp in range(2):
        for cp in range(2):
            rows = [
                jnp.concatenate([interp_ref[2 * kp + kk, 2 * cp], interp_ref[2 * kp + kk, 2 * cp + 1]], 1)
                for kk in range(2)
            ]
            high, low = split(jnp.concatenate(rows, 0).T)
            for part, value in enumerate((high, high, low)):
                at = part * WIDE + cp * LANES
                matrix_ref[at : at + LANES, kp * LANES : (kp + 1) * LANES] = value

    tiles = rows_scratch.shape[0] // LANES
    for tile in range(tiles):
        rows = []
        for ref, e in ((exit_vmem, 1), (entry_vmem, 2), (exit_vmem, 2)):
            rows.append(ref[pl.ds(16 * e + tile, 4, stride=tiles), :].astype(jnp.float32))
            rows.append(jnp.zeros((12, LANES), jnp.float32))
        rows.append(jnp.zeros((LANES - 48, LANES), jnp.float32))
        rows_scratch[tile * LANES : (tile + 1) * LANES, :] = jnp.concatenate(rows, 0).T
    lane = lax.broadcasted_iota(jnp.int32, (LANES, LANES), 1)
    indices = rows_scratch[pl.ds(0, LANES, stride=4), :]
    for a in range(1, 4):
        part = pltpu.roll(rows_scratch[pl.ds(a, LANES, stride=4), :], 4 * a, 1)
        indices = jnp.where((lane & 15) >= 4 * a, part, indices)
    out_ref[pl.ds(16, LANES, stride=CHUNK), :] = indices

    def build(p, carry):
        piece(p).wait()

        def block(b, carry):
            at = pl.multiple_of(p * width + b * 2 * LANES, 2 * LANES)
            cos_part, sin_part = cos_sin(travel_ref[:, pl.ds(at, 2 * LANES)])
            table_ref[pl.ds(at, 2 * LANES), :] = jnp.concatenate([cos_part, sin_part], 0).T
            return carry

        return lax.fori_loop(0, width // (2 * LANES), block, carry, unroll=2)

    lax.fori_loop(0, PIECES, build, 0)
    for copy in copies[3:]:
        copy.wait()

    def gather(step, carry):
        for n in range(4):
            at = step * 4 + n
            for group in range(groups):
                wave0[pl.ds(group * LANES + at, 1), :] = table_ref[pl.ds(entry_refs[group][0, at], 1), :]
        return carry

    lax.fori_loop(0, LANES // 4, gather, 0)

    count = tiles * LANES

    def pair(wave, p, at):
        return interleave(
            *[wave[pl.ds(pl.multiple_of(n * count + at, LANES), LANES), :] for n in (2 * p, 2 * p + 1)]
        )

    def enter(tile, carry):
        at = pl.multiple_of(tile * LANES, LANES)
        chunks = iter(range(8))

        def between():
            base = tile * (LANES // tiles) + next(chunks) * (LANES // tiles // 8)
            for n in range(LANES // tiles // 8):
                at = base + n
                for wave, refs in ((wave1, exit_refs), (wave2, next_refs)):
                    for group in range(groups):
                        wave[pl.ds(group * LANES + at, 1), :] = table_ref[pl.ds(refs[group][0, at], 1), :]

        for cx in range(2):
            parts = []
            for r in range(2):
                start = r * HALF * 16 + cx * 8 + tile * 2
                block = [w_ref[pl.ds(start + cy, HALF, stride=16), :] for cy in range(2)]
                parts.append(jnp.concatenate(block, 0).T)
            between()
            real, imag = demodulate(pair(wave0, cx, at), *parts)
            put(x_ref, 0, cx, real)
            put(x_ref, LANES, cx, imag)
            between()
        between()
        merged[pl.ds(pl.multiple_of(tile * WIDE, WIDE), WIDE), :] = dot(x_ref, matrix_ref, between)
        return carry

    lax.fori_loop(0, tiles, enter, 0)

    def leave(tile, carry):
        at = pl.multiple_of(tile * LANES, LANES)
        sent = out_ref.at[pl.ds(pl.multiple_of(tile * (LANES // 4) * CHUNK, 8), (LANES // 4) * CHUNK), :]
        for kp in range(2):
            block = slice(kp * LANES, (kp + 1) * LANES)
            real, imag = [
                merged[pl.ds(pl.multiple_of(tile * WIDE + r * LANES, LANES), LANES), block] for r in range(2)
            ]
            fields = modulate(pair(wave1, kp, at), real, imag)
            fields = demodulate(pair(wave2, kp, at), *fields)
            for r in range(2):
                for n in range(LANES // 4):
                    to = n * CHUNK + r * 8 + kp * 4
                    sent[to : to + 4, :] = fields[r][4 * n : 4 * n + 4, :]
        return carry

    lax.fori_loop(0, tiles, leave, 0)


def target_kernel(
    x_ref, table_ref, matrix_ref,
    out_ref, rows_vmem, waves, more_waves, x1_ref, x2_ref, merged, result, last, sems, *rows_smem,
):
    rows_vmem[...] = x_ref[pl.ds(16, LANES, stride=CHUNK), :].astype(jnp.int32).T
    copies = [
        pltpu.make_async_copy(rows_vmem.at[pl.ds(n, 1), :], to, sems.at[n]) for n, to in enumerate(rows_smem)
    ]
    for copy in copies:
        copy.start()

    bits = range(2)

    def first(step, carry):
        base = 32 * CHUNK
        part = x_ref.at[pl.ds(pl.multiple_of(step * base, 8), base), :]
        for sy in range(4):
            for j1 in bits:
                group = pl.multiple_of(step * 256 + (sy * 2 + j1) * 32, 32)
                for i0 in bits:
                    at = [(i0 * 16 + sy * 4 + j1 * 2 + j0) * CHUNK for j0 in bits]
                    parts = interleave(*[part[a : a + 16, :] for a in at])
                    rows = [parts[kk][8 * r : 8 * r + 8] for r in bits for kk in bits]
                    put(x1_ref, group, i0, jnp.concatenate(rows, 0))
        return carry

    lax.fori_loop(0, 4, first, 0)

    merged[:512, :] = dot(x1_ref.at[:512, :], matrix_ref)
    for copy in copies:
        copy.wait()

    def gather(n, wave):
        base = n // 4 * 64 + n % 4 * 4
        chunks = iter(range(16))

        def chunk():
            b = next(chunks)
            source = base + (b >> 2) * 16 + b % 4
            for e in range(3):
                for k in range(4):
                    for a in range(4):
                        index = rows_smem[e * 16 + a * 4 + k][0, source]
                        at = e * 256 + b * 16 + k % 2 * 8 + k // 2 * 4 + a
                        wave[at : at + 1, :] = table_ref[pl.ds(index, 1), :]

        return chunk

    def levels(n, wave, between):
        sx, sy = n // 4, n % 4

        def pair(to, ends):
            at = [to * 256 + ((i1 * 2 + i0) * 4 + j1 * 2 + j0) * 16 for i1, i0, j1, j0 in ends]
            return interleave(*[wave[a : a + 16, :] for a in at])

        for i1 in bits:
            for i0 in bits:
                fields = []
                block = slice(i0 * LANES, (i0 + 1) * LANES)
                for j1 in bits:
                    group = sx * 512 + sy * 64 + i1 * 256 + j1 * 32
                    field = [
                        merged[pl.ds(pl.multiple_of(group + r * 16, 16), 16), block] for r in bits
                    ]
                    ends = [(i1, i0, j1, j0) for j0 in bits]
                    field = modulate(pair(0, ends), *field)
                    fields.append(demodulate(pair(1, ends), *field))
                for r in bits:
                    parts = interleave(fields[0][r], fields[1][r])
                    for j0 in bits:
                        put(x2_ref, (i0 * 2 + j0) * 32 + r * 16, i1, parts[j0])
                    between()
        result[...] = dot(x2_ref, matrix_ref, between)
        for i0 in bits:
            for j0 in bits:
                for i1 in bits:
                    block = slice(i1 * LANES, (i1 + 1) * LANES)
                    group = (i0 * 2 + j0) * 32
                    field = [result[group + r * 16 : group + r * 16 + 16, block] for r in bits]
                    field = interleave(*modulate(pair(2, [(i1, i0, j1, j0) for j1 in bits]), *field))
                    for j1 in bits:
                        at = (i0 * 8 + j0 * 4 + i1 * 2 + j1) * CHUNK
                        last[at : at + 16, :] = field[j1]
                between()
        for half in bits:
            pieces = [
                last[pl.ds((k % 2) * 8 + (k // 2) * 4 + a, 16, stride=CHUNK), :]
                for a in (2 * half, 2 * half + 1)
                for k in range(4)
            ]
            out_ref[pl.ds(sx * 8 + half * 4 + sy, LANES, stride=16), :] = jnp.concatenate(pieces, 0).T
            if half == 0:
                between()

    chunk = gather(0, waves)

    def some():
        for _ in range(5):
            chunk()

    merged[512:, :] = dot(x1_ref.at[512:, :], matrix_ref, some)
    chunk()

    def two(m, carry):
        levels(2 * m, waves, gather(2 * m + 1, more_waves))
        levels(2 * m + 1, more_waves, gather((2 * m + 2) % 8, waves))
        return carry

    lax.fori_loop(0, 4, two, 0)


def shards(weights, interp, travel, entry_rows, exit_rows):
    count = weights.shape[-1]
    points = interp.shape[-1]
    devices = lax.axis_size("gx") * lax.axis_size("gy")
    slots = 4 * count
    entry = entry_rows.reshape(3 * slots // LANES, LANES)
    exits = exit_rows.reshape(3 * slots // LANES, LANES)
    state = weights.reshape(2 * points, 2, 2, count // LANES, LANES)
    state = state.transpose(0, 1, 3, 2, 4).reshape(slots, LANES)
    f32 = lambda *shape: jax.ShapeDtypeStruct(shape, jnp.float32)
    vmem = lambda *shape: pltpu.VMEM(shape, jnp.float32)
    params = pltpu.CompilerParams(vmem_limit_bytes=28 << 20)
    operands = state, interp, travel, entry, exits
    payload, table, matrix = pl.pallas_call(
        source_kernel,
        out_shape=[
            f32(devices * CHUNK, LANES),
            f32(travel.shape[1], LANES),
            jax.ShapeDtypeStruct((3 * WIDE, WIDE), jnp.bfloat16),
        ],
        in_specs=[HBM] * 5,
        out_specs=[VMEM] * 3,
        scratch_shapes=[
            vmem(slots, LANES),
            vmem(*interp.shape),
            vmem(*travel.shape),
            pltpu.VMEM(entry.shape, jnp.int32),
            pltpu.VMEM(exits.shape, jnp.int32),
            vmem(slots, LANES),
            vmem(slots, LANES),
            vmem(slots, LANES),
            vmem(count, LANES),
            pltpu.VMEM((WIDE, 3 * WIDE), jnp.bfloat16),
            vmem(slots // 2, WIDE),
            pltpu.SemaphoreType.DMA((PIECES + 4 + 48,)),
        ]
        + [pltpu.SMEM((1, LANES), jnp.int32)] * 48,
        compiler_params=params,
        name="source",
    )(*[pltpu.with_memory_space_constraint(x, pltpu.HBM) for x in operands])
    moved = lax.all_to_all(
        payload.reshape(devices, 1, -1), ("gx", "gy"), split_axis=0, concat_axis=0, tiled=True
    )
    out = pl.pallas_call(
        target_kernel,
        out_shape=f32(slots, LANES),
        in_specs=[VMEM] * 3,
        out_specs=VMEM,
        scratch_shapes=[
            pltpu.VMEM((LANES, LANES), jnp.int32),
            vmem(3 * 256, LANES),
            vmem(3 * 256, LANES),
            pltpu.VMEM((slots // 2, 3 * WIDE), jnp.bfloat16),
            pltpu.VMEM((LANES, 3 * WIDE), jnp.bfloat16),
            vmem(slots // 2, WIDE),
            vmem(LANES, WIDE),
            vmem(16 * CHUNK, LANES),
            pltpu.SemaphoreType.DMA((48,)),
        ]
        + [pltpu.SMEM((1, LANES), jnp.int32)] * 48,
        compiler_params=params,
        name="target",
    )(moved.reshape(devices * CHUNK, LANES), table, matrix)
    out = out.reshape(2, points, 2, 2, 4, LANES).transpose(0, 1, 2, 4, 3, 5)
    return out.reshape(2, points, 2, 4, 2 * LANES)


def solution(mesh):
    return jax.shard_map(
        shards,
        mesh=mesh,
        in_specs=(
            P(None, None, "gx", "gy", None),
            P(),
            P(),
            P(None, "gx", "gy", None),
            P(None, "gx", "gy", None),
        ),
        out_specs=P(None, None, None, None, ("gx", "gy")),
        check_vma=False,
    )
```

```python
import jax
import jax.numpy as jnp
from jax import lax
from jax.experimental import pallas as pl
from jax.experimental.pallas import tpu as pltpu
from jax.sharding import PartitionSpec as P

LANES = 128
HALF = 64
CHUNK = 17
WIDE = 256
VMEM = pl.BlockSpec(memory_space=pltpu.VMEM)
HBM = pl.BlockSpec(memory_space=pltpu.HBM)
PIECES = 4


def cos_sin(x):
    z = x * x
    s = SIN[-1]
    for term in SIN[-2::-1]:
        s = s * z + term
    s = s * x
    c = COS[-1]
    for term in COS[-2::-1]:
        c = c * z + term
    return 1.0 - s * s, s * c


SIN = (0.70710677, -0.029462768, 3.682721e-4, -2.1885735e-6, 7.1936523e-9)
COS = (1.4142135, -0.17677669, 3.682845e-3, -3.0689214e-5, 1.3677929e-7, -3.5967443e-10)


def swap(x):
    return pltpu.roll(x, HALF, 1)


def low_half(x):
    return lax.broadcasted_iota(jnp.int32, x.shape, 1) < HALF


def interleave(first, second):
    low = low_half(first)
    moved = swap(jnp.where(low, second, first))
    return jnp.where(low, first, moved), jnp.where(low, moved, second)


def modulate(wave, real, imag):
    cos_part, sin_part = wave
    return cos_part * real - sin_part * imag, sin_part * real + cos_part * imag


def demodulate(wave, real, imag):
    cos_part, sin_part = wave
    return cos_part * real + sin_part * imag, cos_part * imag - sin_part * real


def split(x):
    high = x.astype(jnp.bfloat16)
    low = (x - high.astype(jnp.float32)).astype(jnp.bfloat16)
    return high, low


def put(ref, row, block, x):
    high, low = split(x)
    for part, value in enumerate((high, low, high)):
        at = part * WIDE + block * LANES
        ref[pl.ds(row, x.shape[0]), at : at + LANES] = value


def dot(x_ref, matrix_ref, between=lambda: None):
    total = None
    for part in range(3):
        at = slice(part * WIDE, (part + 1) * WIDE)
        term = jnp.dot(x_ref[:, at], matrix_ref[at, :], preferred_element_type=jnp.float32)
        total = term if total is None else total + term
        between()
    return total


def source_kernel(
    w_hbm, interp_hbm, travel_hbm, entry_hbm, exit_hbm,
    out_ref, table_ref, matrix_ref,
    w_ref, interp_ref, travel_ref, entry_vmem, exit_vmem,
    wave0, wave1, wave2, rows_scratch, x_ref, merged, sems, *index_refs,
):
    groups = wave0.shape[0] // LANES
    width = travel_ref.shape[1] // PIECES

    def piece(p):
        at = (slice(None), pl.ds(pl.multiple_of(p * width, width), width))
        return pltpu.make_async_copy(travel_hbm.at[at], travel_ref.at[at], sems.at[p])

    operands = (
        (interp_hbm, interp_ref),
        (entry_hbm, entry_vmem),
        (exit_hbm, exit_vmem),
        (w_hbm, w_ref),
    )
    rows = [(entry_hbm, n) for n in range(groups)] + [(exit_hbm, n) for n in range(groups)]
    rows += [(entry_hbm, groups + n) for n in range(groups)]
    operands += tuple((ref.at[pl.ds(n, 1), :], to) for (ref, n), to in zip(rows, index_refs))
    entry_refs, exit_refs, next_refs = [index_refs[n * groups : (n + 1) * groups] for n in range(3)]
    copies = [
        pltpu.make_async_copy(*pair, sems.at[PIECES + n]) for n, pair in enumerate(operands)
    ]
    for copy in copies[:3]:
        copy.start()
    for p in range(PIECES):
        piece(p).start()
    for copy in copies[3:]:
        copy.start()

    for copy in copies[:3]:
        copy.wait()
    for kp in range(2):
        for cp in range(2):
            rows = [
                jnp.concatenate([interp_ref[2 * kp + kk, 2 * cp], interp_ref[2 * kp + kk, 2 * cp + 1]], 1)
                for kk in range(2)
            ]
            high, low = split(jnp.concatenate(rows, 0).T)
            for part, value in enumerate((high, high, low)):
                at = part * WIDE + cp * LANES
                matrix_ref[at : at + LANES, kp * LANES : (kp + 1) * LANES] = value

    tiles = rows_scratch.shape[0] // LANES
    for tile in range(tiles):
        rows = []
        for ref, e in ((exit_vmem, 1), (entry_vmem, 2), (exit_vmem, 2)):
            rows.append(ref[pl.ds(16 * e + tile, 4, stride=tiles), :].astype(jnp.float32))
            rows.append(jnp.zeros((12, LANES), jnp.float32))
        rows.append(jnp.zeros((LANES - 48, LANES), jnp.float32))
        rows_scratch[tile * LANES : (tile + 1) * LANES, :] = jnp.concatenate(rows, 0).T
    lane = lax.broadcasted_iota(jnp.int32, (LANES, LANES), 1)
    indices = rows_scratch[pl.ds(0, LANES, stride=4), :]
    for a in range(1, 4):
        part = pltpu.roll(rows_scratch[pl.ds(a, LANES, stride=4), :], 4 * a, 1)
        indices = jnp.where((lane & 15) >= 4 * a, part, indices)
    out_ref[pl.ds(16, LANES, stride=CHUNK), :] = indices

    def build(p, carry):
        piece(p).wait()

        def block(b, carry):
            at = pl.multiple_of(p * width + b * 2 * LANES, 2 * LANES)
            cos_part, sin_part = cos_sin(travel_ref[:, pl.ds(at, 2 * LANES)])
            table_ref[pl.ds(at, 2 * LANES), :] = jnp.concatenate([cos_part, sin_part], 0).T
            return carry

        return lax.fori_loop(0, width // (2 * LANES), block, carry, unroll=2)

    lax.fori_loop(0, PIECES, build, 0)
    for copy in copies[3:]:
        copy.wait()

    def gather(step, carry):
        for n in range(4):
            at = step * 4 + n
            for group in range(groups):
                wave0[pl.ds(group * LANES + at, 1), :] = table_ref[pl.ds(entry_refs[group][0, at], 1), :]
        return carry

    lax.fori_loop(0, LANES // 4, gather, 0)

    count = tiles * LANES

    def pair(wave, p, at):
        return interleave(
            *[wave[pl.ds(pl.multiple_of(n * count + at, LANES), LANES), :] for n in (2 * p, 2 * p + 1)]
        )

    def enter(tile, carry):
        at = pl.multiple_of(tile * LANES, LANES)
        chunks = iter(range(8))

        def between():
            base = tile * (LANES // tiles) + next(chunks) * (LANES // tiles // 8)
            for n in range(LANES // tiles // 8):
                at = base + n
                for wave, refs in ((wave1, exit_refs), (wave2, next_refs)):
                    for group in range(groups):
                        wave[pl.ds(group * LANES + at, 1), :] = table_ref[pl.ds(refs[group][0, at], 1), :]

        for cx in range(2):
            parts = []
            for r in range(2):
                start = r * HALF * 16 + cx * 8 + tile * 2
                block = [w_ref[pl.ds(start + cy, HALF, stride=16), :] for cy in range(2)]
                parts.append(jnp.concatenate(block, 0).T)
            between()
            real, imag = demodulate(pair(wave0, cx, at), *parts)
            put(x_ref, 0, cx, real)
            put(x_ref, LANES, cx, imag)
            between()
        between()
        merged[pl.ds(pl.multiple_of(tile * WIDE, WIDE), WIDE), :] = dot(x_ref, matrix_ref, between)
        return carry

    lax.fori_loop(0, tiles, enter, 0)

    def leave(tile, carry):
        at = pl.multiple_of(tile * LANES, LANES)
        sent = out_ref.at[pl.ds(pl.multiple_of(tile * (LANES // 4) * CHUNK, 8), (LANES // 4) * CHUNK), :]
        for kp in range(2):
            block = slice(kp * LANES, (kp + 1) * LANES)
            real, imag = [
                merged[pl.ds(pl.multiple_of(tile * WIDE + r * LANES, LANES), LANES), block] for r in range(2)
            ]
            fields = modulate(pair(wave1, kp, at), real, imag)
            fields = demodulate(pair(wave2, kp, at), *fields)
            for r in range(2):
                for n in range(LANES // 4):
                    to = n * CHUNK + r * 8 + kp * 4
                    sent[to : to + 4, :] = fields[r][4 * n : 4 * n + 4, :]
        return carry

    lax.fori_loop(0, tiles, leave, 0)


def target_kernel(
    x_ref, table_ref, matrix_ref,
    out_ref, rows_vmem, waves, more_waves, x1_ref, x2_ref, merged, result, last, sems, *rows_smem,
):
    rows_vmem[...] = x_ref[pl.ds(16, LANES, stride=CHUNK), :].astype(jnp.int32).T
    copies = [
        pltpu.make_async_copy(rows_vmem.at[pl.ds(n, 1), :], to, sems.at[n]) for n, to in enumerate(rows_smem)
    ]
    for copy in copies:
        copy.start()

    bits = range(2)

    def first(step, carry):
        base = 32 * CHUNK
        part = x_ref.at[pl.ds(pl.multiple_of(step * base, 8), base), :]
        for sy in range(4):
            for j1 in bits:
                group = pl.multiple_of(step * 256 + (sy * 2 + j1) * 32, 32)
                for i0 in bits:
                    at = [(i0 * 16 + sy * 4 + j1 * 2 + j0) * CHUNK for j0 in bits]
                    parts = interleave(*[part[a : a + 16, :] for a in at])
                    rows = [parts[kk][8 * r : 8 * r + 8] for r in bits for kk in bits]
                    put(x1_ref, group, i0, jnp.concatenate(rows, 0))
        return carry

    lax.fori_loop(0, 2, first, 0, unroll=2)
    steps = iter((2, 3))

    def rest():
        for step in steps:
            first(jnp.int32(step), 0)
            break


    merged[:512, :] = dot(x1_ref.at[:512, :], matrix_ref, rest)
    for copy in copies:
        copy.wait()

    def gather(n, wave):
        base = n // 4 * 64 + n % 4 * 4
        chunks = iter(range(16))

        def chunk():
            b = next(chunks)
            source = base + (b >> 2) * 16 + b % 4
            for e in range(3):
                for k in range(4):
                    for a in range(4):
                        index = rows_smem[e * 16 + a * 4 + k][0, source]
                        at = e * 256 + b * 16 + k % 2 * 8 + k // 2 * 4 + a
                        wave[at : at + 1, :] = table_ref[pl.ds(index, 1), :]

        return chunk

    def levels(n, wave, between):
        sx, sy = n // 4, n % 4

        def pair(to, ends):
            at = [to * 256 + ((i1 * 2 + i0) * 4 + j1 * 2 + j0) * 16 for i1, i0, j1, j0 in ends]
            return interleave(*[wave[a : a + 16, :] for a in at])

        for i1 in bits:
            for i0 in bits:
                fields = []
                block = slice(i0 * LANES, (i0 + 1) * LANES)
                for j1 in bits:
                    group = sx * 512 + sy * 64 + i1 * 256 + j1 * 32
                    field = [
                        merged[pl.ds(pl.multiple_of(group + r * 16, 16), 16), block] for r in bits
                    ]
                    ends = [(i1, i0, j1, j0) for j0 in bits]
                    field = modulate(pair(0, ends), *field)
                    fields.append(demodulate(pair(1, ends), *field))
                for r in bits:
                    parts = interleave(fields[0][r], fields[1][r])
                    for j0 in bits:
                        put(x2_ref, (i0 * 2 + j0) * 32 + r * 16, i1, parts[j0])
                    between()
        result[...] = dot(x2_ref, matrix_ref, between)
        for i0 in bits:
            for j0 in bits:
                for i1 in bits:
                    block = slice(i1 * LANES, (i1 + 1) * LANES)
                    group = (i0 * 2 + j0) * 32
                    field = [result[group + r * 16 : group + r * 16 + 16, block] for r in bits]
                    field = interleave(*modulate(pair(2, [(i1, i0, j1, j0) for j1 in bits]), *field))
                    for j1 in bits:
                        at = (i0 * 8 + j0 * 4 + i1 * 2 + j1) * CHUNK
                        last[at : at + 16, :] = field[j1]
                between()
        for half in bits:
            pieces = [
                last[pl.ds((k % 2) * 8 + (k // 2) * 4 + a, 16, stride=CHUNK), :]
                for a in (2 * half, 2 * half + 1)
                for k in range(4)
            ]
            out_ref[pl.ds(sx * 8 + half * 4 + sy, LANES, stride=16), :] = jnp.concatenate(pieces, 0).T
            if half == 0:
                between()

    chunk = gather(0, waves)

    def some():
        for _ in range(5):
            chunk()

    merged[512:, :] = dot(x1_ref.at[512:, :], matrix_ref, some)
    chunk()

    def two(m, carry):
        levels(2 * m, waves, gather(2 * m + 1, more_waves))
        levels(2 * m + 1, more_waves, gather((2 * m + 2) % 8, waves))
        return carry

    lax.fori_loop(0, 4, two, 0)


def shards(weights, interp, travel, entry_rows, exit_rows):
    count = weights.shape[-1]
    points = interp.shape[-1]
    devices = lax.axis_size("gx") * lax.axis_size("gy")
    slots = 4 * count
    entry = entry_rows.reshape(3 * slots // LANES, LANES)
    exits = exit_rows.reshape(3 * slots // LANES, LANES)
    state = weights.reshape(2 * points, 2, 2, count // LANES, LANES)
    state = state.transpose(0, 1, 3, 2, 4).reshape(slots, LANES)
    f32 = lambda *shape: jax.ShapeDtypeStruct(shape, jnp.float32)
    vmem = lambda *shape: pltpu.VMEM(shape, jnp.float32)
    params = pltpu.CompilerParams(vmem_limit_bytes=28 << 20)
    operands = state, interp, travel, entry, exits
    payload, table, matrix = pl.pallas_call(
        source_kernel,
        out_shape=[
            f32(devices * CHUNK, LANES),
            f32(travel.shape[1], LANES),
            jax.ShapeDtypeStruct((3 * WIDE, WIDE), jnp.bfloat16),
        ],
        in_specs=[HBM] * 5,
        out_specs=[VMEM] * 3,
        scratch_shapes=[
            vmem(slots, LANES),
            vmem(*interp.shape),
            vmem(*travel.shape),
            pltpu.VMEM(entry.shape, jnp.int32),
            pltpu.VMEM(exits.shape, jnp.int32),
            vmem(slots, LANES),
            vmem(slots, LANES),
            vmem(slots, LANES),
            vmem(count, LANES),
            pltpu.VMEM((WIDE, 3 * WIDE), jnp.bfloat16),
            vmem(slots // 2, WIDE),
            pltpu.SemaphoreType.DMA((PIECES + 4 + 48,)),
        ]
        + [pltpu.SMEM((1, LANES), jnp.int32)] * 48,
        compiler_params=params,
        name="source",
    )(*[pltpu.with_memory_space_constraint(x, pltpu.HBM) for x in operands])
    moved = lax.all_to_all(
        payload.reshape(devices, 1, -1), ("gx", "gy"), split_axis=0, concat_axis=0, tiled=True
    )
    out = pl.pallas_call(
        target_kernel,
        out_shape=f32(slots, LANES),
        in_specs=[VMEM] * 3,
        out_specs=VMEM,
        scratch_shapes=[
            pltpu.VMEM((LANES, LANES), jnp.int32),
            vmem(3 * 256, LANES),
            vmem(3 * 256, LANES),
            pltpu.VMEM((slots // 2, 3 * WIDE), jnp.bfloat16),
            pltpu.VMEM((LANES, 3 * WIDE), jnp.bfloat16),
            vmem(slots // 2, WIDE),
            vmem(LANES, WIDE),
            vmem(16 * CHUNK, LANES),
            pltpu.SemaphoreType.DMA((48,)),
        ]
        + [pltpu.SMEM((1, LANES), jnp.int32)] * 48,
        compiler_params=params,
        name="target",
    )(moved.reshape(devices * CHUNK, LANES), table, matrix)
    out = out.reshape(2, points, 2, 2, 4, LANES).transpose(0, 1, 2, 4, 3, 5)
    return out.reshape(2, points, 2, 4, 2 * LANES)


def solution(mesh):
    return jax.shard_map(
        shards,
        mesh=mesh,
        in_specs=(
            P(None, None, "gx", "gy", None),
            P(),
            P(),
            P(None, "gx", "gy", None),
            P(None, "gx", "gy", None),
        ),
        out_specs=P(None, None, None, None, ("gx", "gy")),
        check_vma=False,
    )
```
